32 devices in a mesh: wav: 8 (over y, x, core), lev: 4 (over z).
Axes of the slice: x: 2, y: 2, z: 4, core: 2. Of those that a mesh axis runs over, the one named last changes fastest.
Arguments:
- spectral: bfloat16 [200, 401, 512], P('wav', None, 'lev'), may hold values from -0.1796875 to 0.1796875
- legendre: bfloat16 [200, 401, 64], P('wav', None, 'lev'), may hold values from -0.4375 to 0.4375
- wave_pair: int32 [200], replicated, may hold values from -1 to 199, as said below
- lat_slot: int32 [64], replicated, may hold values from 0 to 799, as said below
Outputs:
- gridded: bfloat16 [64, 256, 1616], P('wav', 'lev')
The draws below stay inside these ranges and needn't reach their ends.
Inputs may be any that keep to these rules, and one draw needn't show every extreme that they name: `wave_pair`: each pair number 0 to 199 appears exactly once; all other entries are -1. `lat_slot`: the entries are distinct latitudes.
All inputs are finite; a program needn't handle non-finite values.
Results may differ from the reference program's by a relative error of at most 0.0055.
Values may be sent and summed in bfloat16 or wider, within the bound.
A program may use at most 64 MiB of HBM per device.

```python
import math
import jax
import jax.numpy as jnp
from jax import lax

WAVES = 400
NLAT = 800
PAIRS = 200
FOLD = 401
WSLOTS = 200
NROWS = 64
LAYERS = 256


def draw_wave_pair(key, part):
    order = jax.random.permutation(jax.random.fold_in(key, 11), WSLOTS)
    return jnp.where(order < PAIRS, order, -1).astype(jnp.int32)


def draw_lat_slot(key, part):
    order = jax.random.permutation(jax.random.fold_in(key, 13), NLAT)
    return order[:NROWS].astype(jnp.int32)


def levels(own_key, extent, shards, least, high):
    gain = 1.0
    for dim, parts in shards:
        heights = jax.random.uniform(jax.random.fold_in(jax.random.fold_in(own_key, 6), dim), (parts,), jnp.float32, least / len(shards), high / len(shards))
        gain = gain * jnp.repeat(jnp.exp(heights), extent[dim] // parts).reshape((-1,) + (1,) * (len(extent) - 1 - dim))
    return gain


def noise(stream_key, shape, scale, bound, pieces=(), kind=jnp.bfloat16):
    entries = scale * jax.random.normal(stream_key, shape, jnp.float32)
    if pieces:
        entries = entries * levels(stream_key, shape, pieces, -0.22, 0.18)
    return jnp.clip(entries, -bound, bound).astype(kind)


def setup_inputs(seed: int = 0) -> dict:
    seeds = jax.random.split(jax.random.key(seed), 5)
    spectral = noise(seeds[0], (WSLOTS, FOLD, 2 * LAYERS), 0.03, 0.1796875, ((0, 8), (2, 4)))
    legendre = noise(seeds[1], (WSLOTS, FOLD, NROWS), (WAVES // 2) ** -0.5, 0.4375, ((0, 8), (2, 4)))
    wave_pair = draw_wave_pair(jax.random.fold_in(seeds[4], 71), 0)
    lat_slot = draw_lat_slot(jax.random.fold_in(seeds[4], 71), 0)
    return {"spectral": spectral, "legendre": legendre, "wave_pair": wave_pair, "lat_slot": lat_slot}


def fold_masks(pair_ids, fold_count, wave_count):
    fold_rows = jnp.arange(fold_count, dtype=jnp.int32)
    filled = pair_ids >= 0
    border = wave_count - pair_ids
    lower = filled[:, None] & (fold_rows[None, :] < border[:, None])
    upper = filled[:, None] & (fold_rows[None, :] >= border[:, None])
    return jnp.stack([lower, upper], axis=1)


def trig_parts(wave_numbers, steps, counts_b):
    residue = (wave_numbers[None, None] * steps[None, :, None, None]) % counts_b
    angles = residue.astype(jnp.float32) * (2.0 * math.pi) / counts_b.astype(jnp.float32)
    return jnp.cos(angles), jnp.sin(angles)


def synthesis_table(pair_ids, row_lats, lat_count, lon_width, wave_count):
    filled = pair_ids >= 0
    wave_numbers = jnp.stack([pair_ids, wave_count - 1 - pair_ids], axis=1)
    lon_count = 20 + 4 * jnp.minimum(row_lats, lat_count - 1 - row_lats)
    highest = jnp.minimum(wave_count - 1, (lon_count - 1) // 2)
    counts_b = lon_count[:, None, None, None]
    coarse_count = (lon_width + 63) // 64
    coarse_steps = jnp.arange(coarse_count, dtype=jnp.int32) * 64
    fine_steps = jnp.arange(64, dtype=jnp.int32)
    cos_coarse, sin_coarse = trig_parts(wave_numbers, coarse_steps, counts_b)
    cos_fine, sin_fine = trig_parts(wave_numbers, fine_steps, counts_b)
    cos_all = cos_coarse[:, :, None] * cos_fine[:, None] - sin_coarse[:, :, None] * sin_fine[:, None]
    sin_all = sin_coarse[:, :, None] * cos_fine[:, None] + cos_coarse[:, :, None] * sin_fine[:, None]
    row_total = row_lats.shape[0]
    cos_all = cos_all.reshape(row_total, coarse_count * 64, wave_numbers.shape[0], 2)[:, :lon_width]
    sin_all = sin_all.reshape(row_total, coarse_count * 64, wave_numbers.shape[0], 2)[:, :lon_width]
    columns = jnp.arange(lon_width, dtype=jnp.int32)
    valid = filled[None, None, :, None] & (wave_numbers[None, None] <= highest[:, None, None, None]) & (columns[None, :, None, None] < counts_b)
    factor = jnp.where(wave_numbers == 0, 1.0, 2.0).astype(jnp.float32)[None, None]
    real_part = jnp.where(valid, factor * cos_all, 0.0)
    imag_part = jnp.where(valid, -factor * sin_all, 0.0)
    return jnp.stack([real_part, imag_part], axis=-1).astype(jnp.bfloat16)


def reference(spectral, legendre, wave_pair, lat_slot):
    fold_count = spectral.shape[1]
    wave_count = fold_count - 1
    lat_count = NLAT
    lon_width = 2 * lat_count + 16
    layer_count = spectral.shape[2] // 2
    row_total = lat_slot.shape[0]
    half_masks = fold_masks(wave_pair, fold_count, wave_count)
    paired = spectral.reshape(spectral.shape[0], fold_count, layer_count, 2)

    def per_slot(args):
        coefficients, weights, masks_one = args
        masked = jnp.where(masks_one[:, :, None, None], coefficients.astype(jnp.float32)[None], 0.0)
        summed = jnp.einsum("htlc,ta->ahcl", masked, weights.astype(jnp.float32))
        return summed.astype(jnp.bfloat16)

    fourier = lax.map(per_slot, (paired, legendre, half_masks))

    def per_row(args):
        latitude, position = args
        basis = synthesis_table(wave_pair, latitude[None], lat_count, lon_width, wave_count)[0]
        picked = jnp.take(fourier, position, axis=1)
        flat_basis = basis.reshape(lon_width, -1).astype(jnp.float32)
        flat_values = picked.reshape(-1, layer_count).astype(jnp.float32)
        result = jnp.dot(flat_basis, flat_values, preferred_element_type=jnp.float32)
        return result.T.astype(jnp.bfloat16)

    positions = jnp.arange(row_total, dtype=jnp.int32)
    return lax.map(per_row, (lat_slot, positions))
```

```python
import functools
import math

import jax
import jax.numpy as jnp
from jax import lax
from jax.experimental import pallas as pl
from jax.experimental.pallas import tpu as pltpu
from jax.sharding import PartitionSpec as P

NLAT = 800
CH = 16
LANE = 128
KB = 64


def half_turn(x):
    u = x * math.pi
    v = u * u
    s = -2.5052108385441720e-08
    for coef in (2.7557319223985893e-06, -1.9841269841269841e-04, 8.3333333333333333e-03, -1.6666666666666667e-01, 1.0):
        s = s * v + coef
    s = s * u
    c = -2.7557319223985888e-07
    for coef in (2.4801587301587302e-05, -1.3888888888888889e-03, 4.1666666666666667e-02, -0.5, 1.0):
        c = c * v + coef
    return 1.0 - 2.0 * s * s, 2.0 * s * c


def trig(prod, count, inv):
    r = prod - jnp.floor(prod * inv + 0.5) * count
    return half_turn(r * inv)


def kernel(
    nw, nl, slots, wave_count, half_width,
    wp_ref, lat_ref, meven_ref, perm_ref, spec_ref, leg_ref, out_ref,
    spec, leg, stage, snd, rcv, basis, obuf,
    loc_sem, ag_send, ag_recv, aa_send, aa_recv, own_sem, out_sem,
):
    wi = lax.axis_index("wav")
    li = lax.axis_index("lev")
    chunks = snd.shape[0]
    rows = obuf.shape[0]
    fold = spec.shape[1]
    layers = obuf.shape[1]
    width = out_ref.shape[2]
    kdim = chunks * nw * CH
    blocks = half_width // LANE
    qtot = nw * rows
    fmt = pl.DeviceIdType.MESH

    spec_copy = pltpu.make_async_copy(spec_ref, spec, loc_sem.at[0])
    spec_copy.start()
    leg_copy = pltpu.make_async_copy(leg_ref, leg.at[li], loc_sem.at[1])
    leg_copy.start()

    barrier = pltpu.get_barrier_semaphore()
    for d in range(1, nl):
        pl.semaphore_signal(barrier, inc=1, device_id=(wi, lax.rem(li + d, nl)), device_id_type=fmt)
    for d in range(1, nw):
        pl.semaphore_signal(barrier, inc=1, device_id=(lax.rem(wi + d, nw), li), device_id_type=fmt)
    pl.semaphore_wait(barrier, nl - 1 + nw - 1)

    def ag(c, d):
        lo, hi = c * CH, min(slots, (c + 1) * CH)
        return pltpu.make_async_remote_copy(
            src_ref=leg_ref.at[pl.ds(lo, hi - lo)],
            dst_ref=leg.at[li, pl.ds(lo, hi - lo)],
            send_sem=ag_send.at[c, d],
            recv_sem=ag_recv.at[c, d],
            device_id=(wi, lax.rem(li + d, nl)),
            device_id_type=fmt,
        )

    def aa(c, d):
        dest = lax.rem(wi + d, nw)
        return pltpu.make_async_remote_copy(
            src_ref=snd.at[c, dest],
            dst_ref=rcv.at[c, wi],
            send_sem=aa_send.at[c, d],
            recv_sem=aa_recv.at[c, d],
            device_id=(dest, li),
            device_id_type=fmt,
        )

    for c in range(chunks):
        for d in range(1, nl):
            ag(c, d).start()

    fine = lax.broadcasted_iota(jnp.int32, (KB, LANE), 1).astype(jnp.float32)

    def make_basis(step, carry):
        r = lax.div(step, kdim // KB)
        k0 = pl.multiple_of(lax.rem(step, kdim // KB) * KB, KB)
        lat = lat_ref[wi * rows + r]
        count_i = 20 + 4 * jnp.minimum(lat, NLAT - 1 - lat)
        highest = jnp.minimum(wave_count - 1, lax.shift_right_logical(count_i - 1, 1)).astype(jnp.float32)
        count = jnp.full((KB, LANE), count_i.astype(jnp.float32), jnp.float32)
        inv = 1.0 / count
        m_even = meven_ref[pl.ds(k0, KB), :]
        for par in range(2):
            m = m_even if par == 0 else (wave_count - 1.0) - m_even
            amp = jnp.where((m >= 0.0) & (m <= highest), jnp.where(m == 0.0, 1.0, 2.0), 0.0)
            cf, sf = trig(m * fine, count, inv)
            cc, sc = trig(m * (fine * LANE), count, inv)
            cc = cc * amp
            sc = sc * amp
            for b in range(blocks):
                cb = cc[:, b : b + 1]
                sb = sc[:, b : b + 1]
                cols = slice(b * LANE, (b + 1) * LANE)
                basis[r, par, pl.ds(k0, KB), cols] = (cb * cf - sb * sf).astype(jnp.bfloat16)
                basis[r, par, pl.ds(kdim + k0, KB), cols] = (-(sb * cf + cb * sf)).astype(jnp.bfloat16)
        return carry

    def basis_rows(lo, hi):
        lax.fori_loop(lo * (kdim // KB), hi * (kdim // KB), make_basis, 0)

    stage[...] = jnp.zeros_like(stage)
    cols = lax.broadcasted_iota(jnp.int32, (1, fold), 1)

    def fourier(c):
        lo, hi = c * CH, min(slots, (c + 1) * CH)

        def one(i, carry):
            s = lo + i
            p = wp_ref[wi * slots + s]
            low = jnp.where(cols < wave_count - p, 1, 0)
            par = jnp.bitwise_and(p, 1)
            even = jnp.where(low != par, 1.0, 0.0).astype(jnp.bfloat16)
            lg = leg[:, pl.ds(s, 1)].reshape(qtot, fold)
            lg_even = lg * even
            both = jnp.concatenate([lg_even, lg - lg_even], axis=0)
            f = jnp.dot(both, spec[s], preferred_element_type=jnp.float32).astype(jnp.bfloat16)
            g = jnp.dot(f, perm_ref[...], preferred_element_type=jnp.float32)
            for h in range(2):
                stage[pl.ds(h * CH + i, qtot, stride=2 * CH), :] = g[h * qtot : (h + 1) * qtot]
            return carry

        lax.fori_loop(0, hi - lo, one, 0)
        snd[c] = stage[...].astype(jnp.bfloat16).reshape(snd.shape[1:])

    spec_copy.wait()
    leg_copy.wait()
    done = 0
    own = []
    for c in range(chunks):
        upto = rows * (c + 1) // chunks
        basis_rows(done, upto)
        done = upto
        for d in range(1, nl):
            ag(c, d).wait_recv()
        fourier(c)
        for d in range(1, nw):
            aa(c, d).start()
        keep = pltpu.make_async_copy(snd.at[c, wi], rcv.at[c, wi], own_sem.at[c])
        keep.start()
        own.append(keep)

    for c in range(chunks):
        own[c].wait()
        for d in range(1, nw):
            aa(c, d).wait_recv()

    lanes = lax.broadcasted_iota(jnp.int32, (layers, half_width), 1)

    def final(r, carry):
        lat = lat_ref[wi * rows + r]
        half = 10 + 2 * jnp.minimum(lat, NLAT - 1 - lat)
        sums = []
        for par in range(2):
            v = rcv[:, :, r, par].reshape(kdim, 2 * layers)
            vt = v.T
            lhs = jnp.concatenate([vt[:layers], vt[layers:]], axis=1)
            sums.append(jnp.dot(lhs, basis[r, par], preferred_element_type=jnp.float32))
        inside = lanes < half
        first = jnp.where(inside, sums[0] + sums[1], 0.0)
        second = jnp.where(inside, sums[0] - sums[1], 0.0)
        blank = jnp.zeros_like(first)
        moved = pltpu.roll(jnp.concatenate([second, blank], axis=1), half, 1)
        whole = jnp.concatenate([first, blank], axis=1) + moved
        obuf[r] = whole[:, :width].astype(jnp.bfloat16)
        return carry

    lax.fori_loop(0, rows, final, 0)
    out_copy = pltpu.make_async_copy(obuf, out_ref, out_sem)
    out_copy.start()

    for c in range(chunks):
        for d in range(1, nl):
            ag(c, d).wait_send()
        for d in range(1, nw):
            aa(c, d).wait_send()
    out_copy.wait()


def on_device(spectral, legendre, wave_pair, lat_slot):
    slots, fold, items = spectral.shape
    wave_count = fold - 1
    nw = lax.axis_size("wav")
    nl = lax.axis_size("lev")
    rows = lat_slot.shape[0] // nw
    layers = items // 2
    width = 2 * NLAT + 16
    half_width = -(-(width // 2) // LANE) * LANE
    chunks = -(-slots // CH)
    kdim = chunks * nw * CH
    leg_t = jnp.transpose(legendre, (0, 2, 1))
    lrows = leg_t.shape[1]

    pairs = jnp.pad(wave_pair.reshape(nw, slots), ((0, 0), (0, chunks * CH - slots)), constant_values=-1)
    pairs = pairs.reshape(nw, chunks, CH).transpose(1, 0, 2).reshape(kdim)
    m_even = jnp.where(pairs % 2 == 0, pairs, wave_count - 1 - pairs)
    m_even = jnp.where(pairs < 0, -1, m_even).astype(jnp.float32)
    m_even = jnp.broadcast_to(m_even[:, None], (kdim, LANE))
    i = jnp.arange(items)
    perm = (i[:, None] == (2 * (i % layers) + i // layers)[None, :]).astype(jnp.bfloat16)

    vmem = pl.BlockSpec(memory_space=pltpu.VMEM)
    smem = pl.BlockSpec(memory_space=pltpu.SMEM)
    hbm = pl.BlockSpec(memory_space=pl.ANY)
    dma = pltpu.SemaphoreType.DMA
    return pl.pallas_call(
        functools.partial(kernel, nw, nl, slots, wave_count, half_width),
        out_shape=jax.ShapeDtypeStruct((rows, layers, width), jnp.bfloat16),
        in_specs=[smem, smem, vmem, vmem, hbm, hbm],
        out_specs=hbm,
        scratch_shapes=[
            pltpu.VMEM((slots, fold, items), jnp.bfloat16),
            pltpu.VMEM((nl, slots, lrows, fold), jnp.bfloat16),
            pltpu.VMEM((nw * rows * 2 * CH, items), jnp.float32),
            pltpu.VMEM((chunks, nw, rows, 2, CH, items), jnp.bfloat16),
            pltpu.VMEM((chunks, nw, rows, 2, CH, items), jnp.bfloat16),
            pltpu.VMEM((rows, 2, 2 * kdim, half_width), jnp.bfloat16),
            pltpu.VMEM((rows, layers, width), jnp.bfloat16),
            dma((2,)),
            dma((chunks, nl)),
            dma((chunks, nl)),
            dma((chunks, nw)),
            dma((chunks, nw)),
            dma((chunks,)),
            dma,
        ],
        compiler_params=pltpu.CompilerParams(collective_id=0, has_side_effects=True),
    )(wave_pair, lat_slot, m_even, perm, spectral, leg_t)


def solution(mesh):
    return jax.shard_map(
        on_device,
        mesh=mesh,
        in_specs=(P("wav", None, "lev"), P("wav", None, "lev"), P(), P()),
        out_specs=P("wav", "lev", None),
        check_vma=False,
    )
```

```python
import functools
import math

import jax
import jax.numpy as jnp
from jax import lax
from jax.experimental import pallas as pl
from jax.experimental.pallas import tpu as pltpu
from jax.sharding import PartitionSpec as P

NLAT = 800
CH = 16
LANE = 128
KB = 64


def half_turn(x):
    u = x * math.pi
    v = u * u
    s = -2.5052108385441720e-08
    for coef in (2.7557319223985893e-06, -1.9841269841269841e-04, 8.3333333333333333e-03, -1.6666666666666667e-01, 1.0):
        s = s * v + coef
    s = s * u
    c = -2.7557319223985888e-07
    for coef in (2.4801587301587302e-05, -1.3888888888888889e-03, 4.1666666666666667e-02, -0.5, 1.0):
        c = c * v + coef
    return 1.0 - 2.0 * s * s, 2.0 * s * c


def trig(prod, count, inv):
    r = prod - jnp.floor(prod * inv + 0.5) * count
    return half_turn(r * inv)


def kernel(
    nw, nl, slots, wave_count, half_width,
    wp_ref, lat_ref, spec_ref, leg_ref, out_ref,
    spec, own, leg, tail, expand, meven, stage, snd, rcv, basis, obuf,
    loc_sem, ag_send, ag_recv, aa_send, aa_recv, own_sem, out_sem,
):
    wi = lax.axis_index("wav")
    li = lax.axis_index("lev")
    chunks = snd.shape[0]
    rows = obuf.shape[0]
    fold = spec.shape[1]
    main = leg.shape[3]
    rest = fold - main
    per_tile = LANE // rest
    span = (CH // per_tile) * per_tile
    layers = obuf.shape[1]
    items = 2 * layers
    width = out_ref.shape[2]
    kdim = chunks * nw * CH
    blocks = half_width // LANE
    qtot = nw * rows
    fmt = pl.DeviceIdType.MESH
    bounds = [(c * span, min(slots, (c + 1) * span)) for c in range(chunks)]

    own_copy = pltpu.make_async_copy(leg_ref, own, loc_sem.at[0])
    own_copy.start()
    leg_copy = pltpu.make_async_copy(leg_ref.at[:, :, pl.ds(0, main)], leg.at[li], loc_sem.at[1])
    leg_copy.start()
    spec_copy = pltpu.make_async_copy(spec_ref, spec, loc_sem.at[2])
    spec_copy.start()

    barrier = pltpu.get_barrier_semaphore()
    for d in range(1, nl):
        pl.semaphore_signal(barrier, inc=1, device_id=(wi, lax.rem(li + d, nl)), device_id_type=fmt)
    for d in range(1, nw):
        pl.semaphore_signal(barrier, inc=1, device_id=(lax.rem(wi + d, nw), li), device_id_type=fmt)
    pl.semaphore_wait(barrier, nl - 1 + nw - 1)

    def hop(way, k, c, part, block):
        lo, hi = bounds[c]
        if part == 0:
            view = leg.at[block, pl.ds(lo, hi - lo)]
            src = leg_ref.at[pl.ds(lo, hi - lo), :, pl.ds(0, main)] if k == 0 else view
        else:
            view = tail.at[block, c]
            src = view
        return pltpu.make_async_remote_copy(
            src_ref=src,
            dst_ref=view,
            send_sem=ag_send.at[way, k, c, part],
            recv_sem=ag_recv.at[way, k, c, part],
            device_id=(wi, li + 1 - 2 * way),
            device_id_type=fmt,
        )

    def sends(way, k):
        if way == 0:
            return (li - k >= 0) & (li + 1 < nl), jnp.maximum(li - k, 0)
        return (li + k < nl) & (li >= 1), jnp.minimum(li + k, nl - 1)

    def receives(way, k):
        if way == 0:
            return li - 1 - k >= 0, jnp.maximum(li - 1 - k, 0)
        return li + 1 + k < nl, jnp.minimum(li + 1 + k, nl - 1)

    def send(k, c, part):
        for way in range(2):
            going, block = sends(way, k)

            @pl.when(going)
            def _():
                hop(way, k, c, part, block).start()

    def arrive(k, c):
        for way in range(2):
            coming, block = receives(way, k)

            @pl.when(coming)
            def _():
                hop(way, k, c, 0, block).wait_recv()
                hop(way, k, c, 1, block).wait_recv()

        if k + 1 < nl - 1:
            send(k + 1, c, 0)
            send(k + 1, c, 1)

    def aa(c, d):
        dest = lax.rem(wi + d, nw)
        return pltpu.make_async_remote_copy(
            src_ref=snd.at[c, dest],
            dst_ref=rcv.at[c, wi],
            send_sem=aa_send.at[c, d],
            recv_sem=aa_recv.at[c, d],
            device_id=(dest, li),
            device_id_type=fmt,
        )

    for c in range(chunks):
        send(0, c, 0)
    own_copy.wait()
    place_t = lax.broadcasted_iota(jnp.int32, (rest, LANE), 0)
    place_x = lax.broadcasted_iota(jnp.int32, (rest, LANE), 1)
    for c in range(chunks):
        lo, hi = bounds[c]
        for g in range(tail.shape[2]):
            total = jnp.zeros(tail.shape[3:], jnp.float32)
            for n in range(per_tile):
                s = lo + g * per_tile + n
                if s < hi:
                    place = jnp.where(place_x == place_t + n * rest, 1.0, 0.0).astype(jnp.bfloat16)
                    total += jnp.dot(own[s, :, main:], place, preferred_element_type=jnp.float32)
            tail[li, c, g] = total.astype(jnp.bfloat16)
        send(0, c, 1)

    meven[...] = jnp.full_like(meven, -1.0)

    def place_pairs(src, carry):
        for c in range(chunks):
            lo, hi = bounds[c]
            for s in range(lo, hi):
                p = wp_ref[src * slots + s]
                even = jnp.where(jnp.bitwise_and(p, 1) == 0, p, wave_count - 1 - p)
                even = jnp.where(p < 0, -1, even).astype(jnp.float32)
                meven[pl.ds((c * nw + src) * CH + s - lo, 1), :] = jnp.full((1, LANE), even, jnp.float32)
        return carry

    lax.fori_loop(0, nw, place_pairs, 0)
    out_i = lax.broadcasted_iota(jnp.int32, (items, items), 1)
    in_i = lax.broadcasted_iota(jnp.int32, (items, items), 0)
    perm = jnp.where(
        in_i == jnp.where(out_i < layers, 2 * out_i, 2 * (out_i - layers) + 1), 1.0, 0.0
    ).astype(jnp.bfloat16)

    fine = lax.broadcasted_iota(jnp.int32, (KB, LANE), 1).astype(jnp.float32)

    def make_basis(step, carry):
        r = lax.div(step, kdim // KB)
        k0 = pl.multiple_of(lax.rem(step, kdim // KB) * KB, KB)
        lat = lat_ref[wi * rows + r]
        count_i = 20 + 4 * jnp.minimum(lat, NLAT - 1 - lat)
        highest = jnp.minimum(wave_count - 1, lax.shift_right_logical(count_i - 1, 1)).astype(jnp.float32)
        count = jnp.full((KB, LANE), count_i.astype(jnp.float32), jnp.float32)
        inv = 1.0 / count
        m_even = meven[pl.ds(k0, KB), :]
        for par in range(2):
            m = m_even if par == 0 else (wave_count - 1.0) - m_even
            amp = jnp.where((m >= 0.0) & (m <= highest), jnp.where(m == 0.0, 1.0, 2.0), 0.0)
            cf, sf = trig(m * fine, count, inv)
            cc, sc = trig(m * (fine * LANE), count, inv)
            cc = cc * amp
            sc = sc * amp
            for b in range(blocks):
                cb = cc[:, b : b + 1]
                sb = sc[:, b : b + 1]
                cols = slice(b * LANE, (b + 1) * LANE)
                basis[r, par, pl.ds(k0, KB), cols] = (cb * cf - sb * sf).astype(jnp.bfloat16)
                basis[r, par, pl.ds(kdim + k0, KB), cols] = (-(sb * cf + cb * sf)).astype(jnp.bfloat16)
        return carry

    def basis_rows(lo, hi):
        lax.fori_loop(lo * (kdim // KB), hi * (kdim // KB), make_basis, 0)

    stage[...] = jnp.zeros_like(stage)
    cols = lax.broadcasted_iota(jnp.int32, (1, main), 1)
    tcols = lax.broadcasted_iota(jnp.int32, (1, LANE), 1)
    back_x = lax.broadcasted_iota(jnp.int32, (LANE, rest), 0)
    back_t = lax.broadcasted_iota(jnp.int32, (LANE, rest), 1)

    spec_copy.wait()
    for c in range(chunks):
        lo, hi = bounds[c]

        def widen(i, carry):
            n = lax.rem(i, per_tile)
            back = jnp.where(back_x == back_t + n * rest, 1.0, 0.0).astype(jnp.bfloat16)
            expand[lo + i] = jnp.dot(
                back, spec[lo + i, main:, :], preferred_element_type=jnp.float32
            ).astype(jnp.bfloat16)
            return carry

        lax.fori_loop(0, hi - lo, widen, 0)

    def fourier(c):
        lo, hi = bounds[c]

        def one(i, carry):
            s = lo + i
            p = wp_ref[wi * slots + s]
            par = jnp.bitwise_and(p, 1)
            border = wave_count - p

            def split(values, fold_rows):
                low = jnp.where(fold_rows < border, 1, 0)
                even = jnp.where(low != par, 1.0, 0.0).astype(jnp.bfloat16)
                picked = values * even
                return jnp.concatenate([picked, values - picked], axis=0)

            lg = split(leg[:, pl.ds(s, 1)].reshape(qtot, main), cols)
            tile = tail[:, c, pl.ds(lax.div(i, per_tile), 1)].reshape(qtot, LANE)
            lt = split(tile, main + tcols - lax.rem(i, per_tile) * rest)
            f = jnp.dot(lg, spec[s, :main, :], preferred_element_type=jnp.float32)
            f = f + jnp.dot(lt, expand[s], preferred_element_type=jnp.float32)
            g = jnp.dot(f.astype(jnp.bfloat16), perm, preferred_element_type=jnp.float32)
            for h in range(2):
                stage[pl.ds(h * CH + i, qtot, stride=2 * CH), :] = g[h * qtot : (h + 1) * qtot]
            return carry

        lax.fori_loop(0, hi - lo, one, 0)
        snd[c] = stage[...].astype(jnp.bfloat16).reshape(snd.shape[1:])

    leg_copy.wait()
    polls = [(k, c) for k in range(nl - 1) for c in range(chunks)]
    early = len(polls) - chunks
    done = 0
    for n, (k, c) in enumerate(polls[:early]):
        upto = rows * (n + 1) // (early + 1)
        basis_rows(done, upto)
        done = upto
        arrive(k, c)
    basis_rows(done, rows)
    keeps = []
    for c in range(chunks):
        arrive(nl - 2, c)
        fourier(c)
        for d in range(1, nw):
            aa(c, d).start()
        keep = pltpu.make_async_copy(snd.at[c, wi], rcv.at[c, wi], own_sem.at[c])
        keep.start()
        keeps.append(keep)

    for c in range(chunks):
        keeps[c].wait()
        for d in range(1, nw):
            aa(c, d).wait_recv()

    lanes = lax.broadcasted_iota(jnp.int32, (layers, half_width), 1)

    def final(r, carry):
        lat = lat_ref[wi * rows + r]
        half = 10 + 2 * jnp.minimum(lat, NLAT - 1 - lat)
        sums = []
        for par in range(2):
            v = rcv[:, :, r, par].reshape(kdim, 2 * layers)
            vt = v.T
            lhs = jnp.concatenate([vt[:layers], vt[layers:]], axis=1)
            sums.append(jnp.dot(lhs, basis[r, par], preferred_element_type=jnp.float32))
        inside = lanes < half
        first = jnp.where(inside, sums[0] + sums[1], 0.0)
        second = jnp.where(inside, sums[0] - sums[1], 0.0)
        blank = jnp.zeros_like(first)
        moved = pltpu.roll(jnp.concatenate([second, blank], axis=1), half, 1)
        whole = jnp.concatenate([first, blank], axis=1) + moved
        obuf[r] = whole[:, :width].astype(jnp.bfloat16)
        return carry

    lax.fori_loop(0, rows, final, 0)
    out_copy = pltpu.make_async_copy(obuf, out_ref, out_sem)
    out_copy.start()

    for c in range(chunks):
        for k in range(nl - 1):
            for way in range(2):
                going, block = sends(way, k)

                @pl.when(going)
                def _():
                    for part in range(2):
                        hop(way, k, c, part, block).wait_send()

        for d in range(1, nw):
            aa(c, d).wait_send()
    out_copy.wait()


def on_device(spectral, legendre, wave_pair, lat_slot):
    slots, fold, items = spectral.shape
    wave_count = fold - 1
    nw = lax.axis_size("wav")
    nl = lax.axis_size("lev")
    rows = lat_slot.shape[0] // nw
    layers = items // 2
    width = 2 * NLAT + 16
    half_width = -(-(width // 2) // LANE) * LANE
    main = fold // LANE * LANE
    per_tile = LANE // (fold - main)
    span = (CH // per_tile) * per_tile
    chunks = -(-slots // span)
    kdim = chunks * nw * CH
    leg_t = jnp.transpose(legendre, (0, 2, 1))
    lrows = leg_t.shape[1]

    smem = pl.BlockSpec(memory_space=pltpu.SMEM)
    hbm = pl.BlockSpec(memory_space=pl.ANY)
    dma = pltpu.SemaphoreType.DMA
    vmem = pltpu.VMEM
    half = jnp.bfloat16
    return pl.pallas_call(
        functools.partial(kernel, nw, nl, slots, wave_count, half_width),
        out_shape=jax.ShapeDtypeStruct((rows, layers, width), half),
        in_specs=[smem, smem, hbm, hbm],
        out_specs=hbm,
        scratch_shapes=[
            vmem((slots, fold, items), half),
            vmem((slots, lrows, fold), half),
            vmem((nl, slots, lrows, main), half),
            vmem((nl, chunks, CH // per_tile, lrows, LANE), half),
            vmem((slots, LANE, items), half),
            vmem((kdim, LANE), jnp.float32),
            vmem((nw * rows * 2 * CH, items), jnp.float32),
            vmem((chunks, nw, rows, 2, CH, items), half),
            vmem((chunks, nw, rows, 2, CH, items), half),
            vmem((rows, 2, 2 * kdim, half_width), half),
            vmem((rows, layers, width), half),
            dma((3,)),
            dma((2, nl - 1, chunks, 2)),
            dma((2, nl - 1, chunks, 2)),
            dma((chunks, nw)),
            dma((chunks, nw)),
            dma((chunks,)),
            dma,
        ],
        compiler_params=pltpu.CompilerParams(collective_id=0, has_side_effects=True),
    )(wave_pair, lat_slot, spectral, leg_t)


def solution(mesh):
    return jax.shard_map(
        on_device,
        mesh=mesh,
        in_specs=(P("wav", None, "lev"), P("wav", None, "lev"), P(), P()),
        out_specs=P("wav", "lev", None),
        check_vma=False,
    )
```

```python
import functools
import math

import jax
import jax.numpy as jnp
from jax import lax
from jax.experimental import pallas as pl
from jax.experimental.pallas import tpu as pltpu
from jax.sharding import PartitionSpec as P

NLAT = 800
CH = 16
LANE = 128
KB = 64


def half_turn(x):
    u = x * math.pi
    v = u * u
    s = -2.5052108385441720e-08
    for coef in (2.7557319223985893e-06, -1.9841269841269841e-04, 8.3333333333333333e-03, -1.6666666666666667e-01, 1.0):
        s = s * v + coef
    s = s * u
    c = -2.7557319223985888e-07
    for coef in (2.4801587301587302e-05, -1.3888888888888889e-03, 4.1666666666666667e-02, -0.5, 1.0):
        c = c * v + coef
    return 1.0 - 2.0 * s * s, 2.0 * s * c


def trig(prod, count, inv):
    r = prod - jnp.floor(prod * inv + 0.5) * count
    return half_turn(r * inv)


def kernel(
    nw, nl, slots, wave_count, half_width,
    wp_ref, lat_ref, spec_ref, leg_ref, out_ref,
    spec, own, leg, tail, expand, meven, amp, full, part, stage, snd, rcv, basis, obuf,
    loc_sem, ag_send, ag_recv, aa_send, aa_recv, own_sem, out_sem,
):
    wi = lax.axis_index("wav")
    li = lax.axis_index("lev")
    chunks = snd.shape[0]
    rows = obuf.shape[0]
    fold = spec.shape[1]
    main = leg.shape[3]
    rest = fold - main
    per_tile = LANE // rest
    span = (CH // per_tile) * per_tile
    layers = obuf.shape[1]
    items = 2 * layers
    width = out_ref.shape[2]
    kdim = chunks * nw * CH
    blocks = half_width // LANE
    qtot = nw * rows
    fmt = pl.DeviceIdType.MESH
    bounds = [(c * span, min(slots, (c + 1) * span)) for c in range(chunks)]

    own_copy = pltpu.make_async_copy(leg_ref, own, loc_sem.at[0])
    own_copy.start()
    leg_copy = pltpu.make_async_copy(leg_ref.at[:, :, pl.ds(0, main)], leg.at[li], loc_sem.at[1])
    leg_copy.start()
    spec_copy = pltpu.make_async_copy(spec_ref, spec, loc_sem.at[2])
    spec_copy.start()

    barrier = pltpu.get_barrier_semaphore()
    for d in range(1, nl):
        pl.semaphore_signal(barrier, inc=1, device_id=(wi, lax.rem(li + d, nl)), device_id_type=fmt)
    for d in range(1, nw):
        pl.semaphore_signal(barrier, inc=1, device_id=(lax.rem(wi + d, nw), li), device_id_type=fmt)
    pl.semaphore_wait(barrier, nl - 1 + nw - 1)

    def hop(way, k, c, piece, block):
        lo, hi = bounds[c]
        if piece == 0:
            view = leg.at[block, pl.ds(lo, hi - lo)]
            src = leg_ref.at[pl.ds(lo, hi - lo), :, pl.ds(0, main)] if k == 0 else view
        else:
            view = tail.at[block, c]
            src = view
        return pltpu.make_async_remote_copy(
            src_ref=src,
            dst_ref=view,
            send_sem=ag_send.at[way, k, c, piece],
            recv_sem=ag_recv.at[way, k, c, piece],
            device_id=(wi, li + 1 - 2 * way),
            device_id_type=fmt,
        )

    def sends(way, k):
        if way == 0:
            return (li - k >= 0) & (li + 1 < nl), jnp.maximum(li - k, 0)
        return (li + k < nl) & (li >= 1), jnp.minimum(li + k, nl - 1)

    def receives(way, k):
        if way == 0:
            return li - 1 - k >= 0, jnp.maximum(li - 1 - k, 0)
        return li + 1 + k < nl, jnp.minimum(li + 1 + k, nl - 1)

    def send(k, c, piece):
        for way in range(2):
            going, block = sends(way, k)

            @pl.when(going)
            def _():
                hop(way, k, c, piece, block).start()

    def arrive(k, c):
        for way in range(2):
            coming, block = receives(way, k)

            @pl.when(coming)
            def _():
                hop(way, k, c, 0, block).wait_recv()
                hop(way, k, c, 1, block).wait_recv()

        if k + 1 < nl - 1:
            send(k + 1, c, 0)
            send(k + 1, c, 1)

    def aa(c, d):
        dest = lax.rem(wi + d, nw)
        return pltpu.make_async_remote_copy(
            src_ref=snd.at[c, dest],
            dst_ref=rcv.at[c, wi],
            send_sem=aa_send.at[c, d],
            recv_sem=aa_recv.at[c, d],
            device_id=(dest, li),
            device_id_type=fmt,
        )

    for c in range(chunks):
        send(0, c, 0)
    own_copy.wait()
    place_t = lax.broadcasted_iota(jnp.int32, (rest, LANE), 0)
    place_x = lax.broadcasted_iota(jnp.int32, (rest, LANE), 1)
    for c in range(chunks):
        lo, hi = bounds[c]
        for g in range(tail.shape[2]):
            total = jnp.zeros(tail.shape[3:], jnp.float32)
            for n in range(per_tile):
                s = lo + g * per_tile + n
                if s < hi:
                    place = jnp.where(place_x == place_t + n * rest, 1.0, 0.0).astype(jnp.bfloat16)
                    total += jnp.dot(own[s, :, main:], place, preferred_element_type=jnp.float32)
            tail[li, c, g] = total.astype(jnp.bfloat16)
        send(0, c, 1)

    meven[...] = jnp.full_like(meven, -1.0)

    def place_pairs(src, carry):
        for c in range(chunks):
            lo, hi = bounds[c]
            for s in range(lo, hi):
                p = wp_ref[src * slots + s]
                even = jnp.where(jnp.bitwise_and(p, 1) == 0, p, wave_count - 1 - p)
                even = jnp.where(p < 0, -1, even).astype(jnp.float32)
                meven[pl.ds((c * nw + src) * CH + s - lo, 1), :] = jnp.full((1, LANE), even, jnp.float32)
        return carry

    lax.fori_loop(0, nw, place_pairs, 0)
    out_i = lax.broadcasted_iota(jnp.int32, (items, items), 1)
    in_i = lax.broadcasted_iota(jnp.int32, (items, items), 0)
    perm = jnp.where(
        in_i == jnp.where(out_i < layers, 2 * out_i, 2 * (out_i - layers) + 1), 1.0, 0.0
    ).astype(jnp.bfloat16)

    fine = lax.broadcasted_iota(jnp.int32, (KB, LANE), 1).astype(jnp.float32)
    ahead = lax.broadcasted_iota(jnp.int32, (8, half_width), 1).astype(jnp.float32)
    kchunk = nw * CH
    pieces = kdim // KB

    def turn(x, y):
        return x[0] * y[0] - x[1] * y[1], x[0] * y[1] + x[1] * y[0]

    def minus(pair):
        return pair[0], -pair[1]

    def row_count(r):
        lat = lat_ref[wi * rows + r]
        return 20 + 4 * jnp.minimum(lat, NLAT - 1 - lat)

    def make_basis(step, carry):
        r = lax.div(step, pieces)
        k0 = pl.multiple_of(lax.rem(step, pieces) * KB, KB)
        slab = lax.div(k0, kchunk)
        real = pl.multiple_of(k0 + slab * kchunk, KB)
        imag = pl.multiple_of(real + kchunk, KB)
        count_i = row_count(r)
        highest = jnp.minimum(wave_count - 1, lax.shift_right_logical(count_i - 1, 1)).astype(jnp.float32)
        count = jnp.full((KB, LANE), count_i.astype(jnp.float32), jnp.float32)
        inv = 1.0 / count
        m_even = meven[pl.ds(k0, KB), :]
        for par in range(2):
            m = m_even if par == 0 else (wave_count - 1.0) - m_even
            factor = jnp.where((m >= 0.0) & (m <= highest), jnp.where(m == 0.0, 1.0, 2.0), 0.0)
            amp[r, par, pl.ds(k0, KB), :] = factor.astype(jnp.bfloat16)
        now = minus(trig(m_even * fine, count, inv))
        stride = minus(trig(m_even * LANE, count, inv))
        for b in range(blocks):
            cols = slice(b * LANE, (b + 1) * LANE)
            if b:
                now = turn(now, stride)
            c4 = jnp.broadcast_to(full[r, 0, 0:1, cols], (KB, LANE))
            s4 = jnp.broadcast_to(full[r, 1, 0:1, cols], (KB, LANE))
            basis[r, 0, pl.ds(real, KB), cols] = now[0].astype(jnp.bfloat16)
            basis[r, 0, pl.ds(imag, KB), cols] = now[1].astype(jnp.bfloat16)
            other = (c4 * now[0] + s4 * now[1], s4 * now[0] - c4 * now[1])
            basis[r, 1, pl.ds(real, KB), cols] = other[0].astype(jnp.bfloat16)
            basis[r, 1, pl.ds(imag, KB), cols] = other[1].astype(jnp.bfloat16)
        return carry

    def make_full(r, carry):
        count = jnp.full((8, half_width), row_count(r).astype(jnp.float32), jnp.float32)
        cos_full, neg_sin_full = minus(trig((wave_count - 1.0) * ahead, count, 1.0 / count))
        full[r, 0] = cos_full
        full[r, 1] = neg_sin_full
        return carry

    lax.fori_loop(0, rows, make_full, 0)

    def basis_rows(lo, hi):
        lax.fori_loop(lo * pieces, hi * pieces, make_basis, 0)

    stage[...] = jnp.zeros_like(stage)
    cols = lax.broadcasted_iota(jnp.int32, (1, main), 1)
    tcols = lax.broadcasted_iota(jnp.int32, (1, LANE), 1)
    back_x = lax.broadcasted_iota(jnp.int32, (LANE, rest), 0)
    back_t = lax.broadcasted_iota(jnp.int32, (LANE, rest), 1)

    spec_copy.wait()
    for c in range(chunks):
        lo, hi = bounds[c]

        def widen(i, carry):
            n = lax.rem(i, per_tile)
            back = jnp.where(back_x == back_t + n * rest, 1.0, 0.0).astype(jnp.bfloat16)
            expand[lo + i] = jnp.dot(
                back, spec[lo + i, main:, :], preferred_element_type=jnp.float32
            ).astype(jnp.bfloat16)
            return carry

        lax.fori_loop(0, hi - lo, widen, 0)

    def fourier(c):
        lo, hi = bounds[c]

        for i in range(hi - lo):
            s = lo + i
            p = wp_ref[wi * slots + s]
            par = jnp.bitwise_and(p, 1)
            border = wave_count - p

            def split(values, fold_rows):
                low = jnp.where(fold_rows < border, 1, 0)
                even = jnp.where(low != par, 1.0, 0.0).astype(jnp.bfloat16)
                picked = values * even
                return jnp.concatenate([picked, values - picked], axis=0)

            lg = split(leg[:, s].reshape(qtot, main), cols)
            tile = tail[:, c, i // per_tile].reshape(qtot, LANE)
            lt = split(tile, main + tcols - i % per_tile * rest)
            f = jnp.dot(lg, spec[s, :main, :], preferred_element_type=jnp.float32)
            f = f + jnp.dot(lt, expand[s], preferred_element_type=jnp.float32)
            g = jnp.dot(f.astype(jnp.bfloat16), perm, preferred_element_type=jnp.float32)
            for h in range(2):
                stage[pl.ds(h * CH + i, qtot, stride=2 * CH), :] = g[h * qtot : (h + 1) * qtot]

        snd[c] = stage[...].astype(jnp.bfloat16).reshape(snd.shape[1:])

    leg_copy.wait()
    polls = [(k, c) for k in range(nl - 1) for c in range(chunks)]
    early = len(polls) - chunks
    done = 0
    for n, (k, c) in enumerate(polls[:early]):
        upto = rows * (n + 1) // (early + 1)
        basis_rows(done, upto)
        done = upto
        arrive(k, c)
    basis_rows(done, rows)
    keeps = []
    for c in range(chunks):
        arrive(nl - 2, c)
        fourier(c)
        for d in range(1, nw):
            aa(c, d).start()
        keep = pltpu.make_async_copy(snd.at[c, wi], rcv.at[c, wi], own_sem.at[c])
        keep.start()
        keeps.append(keep)

    def landed(c):
        keeps[c].wait()
        for d in range(1, nw):
            aa(c, d).wait_recv()

    def product(c, r, par):
        weight = amp[r, par, c * kchunk : (c + 1) * kchunk, :]
        v = rcv[c, :, r, par].reshape(kchunk, items) * weight
        vt = v.T
        lhs = jnp.concatenate([vt[:layers], vt[layers:]], axis=1)
        rhs = basis[r, par, 2 * c * kchunk : 2 * (c + 1) * kchunk, :]
        return jnp.dot(lhs, rhs, preferred_element_type=jnp.float32)

    for c in range(chunks - 1):
        landed(c)

        def partial(r, carry):
            for par in range(2):
                value = product(c, r, par)
                part[r, par] = value if c == 0 else part[r, par] + value
            return carry

        lax.fori_loop(0, rows, partial, 0)

    lanes = lax.broadcasted_iota(jnp.int32, (layers, half_width), 1)
    landed(chunks - 1)

    def final(r, carry):
        half = lax.shift_right_logical(row_count(r), 1)
        sums = []
        for par in range(2):
            value = product(chunks - 1, r, par)
            sums.append(value if chunks == 1 else part[r, par] + value)
        inside = lanes < half
        first = jnp.where(inside, sums[0] + sums[1], 0.0)
        second = jnp.where(inside, sums[0] - sums[1], 0.0)
        blank = jnp.zeros_like(first)
        moved = pltpu.roll(jnp.concatenate([second, blank], axis=1), half, 1)
        whole = jnp.concatenate([first, blank], axis=1) + moved
        obuf[r] = whole[:, :width].astype(jnp.bfloat16)
        return carry

    lax.fori_loop(0, rows, final, 0)
    out_copy = pltpu.make_async_copy(obuf, out_ref, out_sem)
    out_copy.start()

    for c in range(chunks):
        for k in range(nl - 1):
            for way in range(2):
                going, block = sends(way, k)

                @pl.when(going)
                def _():
                    for piece in range(2):
                        hop(way, k, c, piece, block).wait_send()

        for d in range(1, nw):
            aa(c, d).wait_send()
    out_copy.wait()


def on_device(spectral, legendre, wave_pair, lat_slot):
    slots, fold, items = spectral.shape
    wave_count = fold - 1
    nw = lax.axis_size("wav")
    nl = lax.axis_size("lev")
    rows = lat_slot.shape[0] // nw
    layers = items // 2
    width = 2 * NLAT + 16
    half_width = -(-(width // 2) // LANE) * LANE
    main = fold // LANE * LANE
    per_tile = LANE // (fold - main)
    span = (CH // per_tile) * per_tile
    chunks = -(-slots // span)
    kdim = chunks * nw * CH
    leg_t = jnp.transpose(legendre, (0, 2, 1))
    lrows = leg_t.shape[1]

    smem = pl.BlockSpec(memory_space=pltpu.SMEM)
    hbm = pl.BlockSpec(memory_space=pl.ANY)
    dma = pltpu.SemaphoreType.DMA
    vmem = pltpu.VMEM
    half = jnp.bfloat16
    return pl.pallas_call(
        functools.partial(kernel, nw, nl, slots, wave_count, half_width),
        out_shape=jax.ShapeDtypeStruct((rows, layers, width), half),
        in_specs=[smem, smem, hbm, hbm],
        out_specs=hbm,
        scratch_shapes=[
            vmem((slots, fold, items), half),
            vmem((slots, lrows, fold), half),
            vmem((nl, slots, lrows, main), half),
            vmem((nl, chunks, CH // per_tile, lrows, LANE), half),
            vmem((slots, LANE, items), half),
            vmem((kdim, LANE), jnp.float32),
            vmem((rows, 2, kdim, LANE), half),
            vmem((rows, 2, 8, half_width), jnp.float32),
            vmem((rows, 2, layers, half_width), jnp.float32),
            vmem((nw * rows * 2 * CH, items), jnp.float32),
            vmem((chunks, nw, rows, 2, CH, items), half),
            vmem((chunks, nw, rows, 2, CH, items), half),
            vmem((rows, 2, 2 * kdim, half_width), half),
            vmem((rows, layers, width), half),
            dma((3,)),
            dma((2, nl - 1, chunks, 2)),
            dma((2, nl - 1, chunks, 2)),
            dma((chunks, nw)),
            dma((chunks, nw)),
            dma((chunks,)),
            dma,
        ],
        compiler_params=pltpu.CompilerParams(collective_id=0, has_side_effects=True),
    )(wave_pair, lat_slot, spectral, leg_t)


def solution(mesh):
    return jax.shard_map(
        on_device,
        mesh=mesh,
        in_specs=(P("wav", None, "lev"), P("wav", None, "lev"), P(), P()),
        out_specs=P("wav", "lev", None),
        check_vma=False,
    )
```
